128 devices in a mesh: dp: 32 (over y, x, core), tensor: 4 (over z).
Axes of the slice: x: 4, y: 4, z: 4, core: 2. Of those that a mesh axis runs over, the one named last changes fastest.
Arguments:
- activations: bfloat16 [32768, 28672], P('dp', 'tensor'), may hold values from -6 to 6
- out_grads: bfloat16 [32768, 8192], P('dp', 'tensor'), may hold values from -6 to 6
- proj_in: bfloat16 [28672, 64], P('tensor'), may hold values from -0.03125 to 0.03125
- proj_out: bfloat16 [8192, 64], P('tensor'), may hold values from -0.0625 to 0.0625
- validation: bfloat16 [512, 4096], P('tensor', 'dp'), may hold values from -0.09375 to 0.09375
- doc_lengths: int32 [32, 32], P('dp'), may hold values from 0 to 1024, as said below
- owner_rows: int32 [32, 32], P('dp'), may hold values from 0 to 1023, as said below
Outputs:
- scores: bfloat16 [1024, 512], P('dp', 'tensor')
The draws below stay inside these ranges and needn't reach their ends.
Inputs may be any that keep to these rules, and one draw needn't show every extreme that they name: `doc_lengths`: in each row the first 1 to 32 entries are positive and sum to 1024, the rest are zero; some row has 32 documents and some row a single document. `owner_rows`: A permutation of 0 to 1024 - 1 over all entries; with owner = row // 32, the slots of one row go to 32 distinct owners, exactly 1 slot to each.
All inputs are finite; a program needn't handle non-finite values.
Results may differ from the reference program's by a relative error of at most 0.0098.
Values may be sent and summed in bfloat16 or wider, within the bound.
A program may use at most 64 MiB of HBM per device.

```python
import jax
import jax.numpy as jnp
from jax import lax

D = 8192
FF = 28672
K = 64
NVAL = 512
TOK_DEV = 1024
MAXDOC = 32
SLOTS = 1
SK = 4096
TOKENS = 32768
N_DP = 32


def draw_doc_lengths(key, part):
    first_key, second_key, third_key = jax.random.split(key, 3)
    counts = jax.random.randint(first_key, (N_DP,), MAXDOC // 2, MAXDOC + 1)
    chosen = jax.random.randint(second_key, (), 0, N_DP)
    rows_index = jnp.arange(N_DP)
    counts = jnp.where(rows_index == chosen, MAXDOC, counts)
    counts = jnp.where(rows_index == (chosen + 1) % N_DP, 1, counts)
    cut_points = jax.vmap(lambda row_key: jax.random.permutation(row_key, TOK_DEV - 1))(jax.random.split(third_key, N_DP)) + 1
    cut_points = cut_points[:, :MAXDOC - 1]
    indices = jnp.arange(MAXDOC - 1)
    cut_points = jnp.where(indices[None, :] < counts[:, None] - 1, cut_points, TOK_DEV)
    sorted_cuts = jnp.sort(cut_points, axis=1)
    boundaries = jnp.concatenate([jnp.zeros((N_DP, 1), jnp.int32), sorted_cuts.astype(jnp.int32), jnp.full((N_DP, 1), TOK_DEV, jnp.int32)], axis=1)
    return (boundaries[:, 1:] - boundaries[:, :-1]).astype(jnp.int32)


def draw_owner_rows(key, part):
    shift_key, slot_key = jax.random.split(jax.random.fold_in(key, 7), 2)
    groups = MAXDOC // SLOTS
    offsets = jax.random.permutation(shift_key, N_DP)[:groups]
    shifts = jax.random.permutation(jax.random.fold_in(shift_key, 1), jnp.repeat(offsets, SLOTS))
    source_perm = jax.random.permutation(jax.random.fold_in(shift_key, 2), N_DP)
    owner_perm = jax.random.permutation(jax.random.fold_in(shift_key, 3), N_DP)
    positions = (source_perm[:, None] + shifts[None, :]) % N_DP
    owners = owner_perm[positions]
    slot_perm = jax.vmap(lambda row_key: jax.random.permutation(row_key, MAXDOC))(jax.random.split(slot_key, N_DP))
    columns = jnp.arange(MAXDOC)
    slots = slot_perm[owners, columns[None, :]]
    return (owners * MAXDOC + slots).astype(jnp.int32)


def steps_of(stream_key, shape, cuts, smallest, largest):
    loudness, own = 1.0, jax.random.fold_in(stream_key, 6)
    for axis_at, parts in cuts:
        heights = jnp.exp(jax.random.uniform(jax.random.fold_in(own, axis_at), (parts,), jnp.float32, smallest / len(cuts), largest / len(cuts)))
        loudness = loudness * jnp.repeat(heights, shape[axis_at] // parts).reshape([-1 if axis == axis_at else 1 for axis in range(len(shape))])
    return loudness


def centred(own_key, dims, deviation, most, cuts=(), kind=jnp.bfloat16):
    loudness = steps_of(own_key, dims, cuts, -0.22, 0.18) if cuts else 1.0
    values = jax.random.normal(own_key, dims, jnp.float32) * deviation * loudness
    return jnp.minimum(jnp.maximum(values, -most), most).astype(kind)


def setup_inputs(seed: int = 0) -> dict:
    key_of = jax.random.split(jax.random.key(seed), 8)
    activations = centred(key_of[0], (TOKENS, FF), 1.0, 6.0, ((0, 32), (1, 4)))
    out_grads = centred(key_of[1], (TOKENS, D), 1.0, 6.0, ((0, 32), (1, 4)))
    proj_in = centred(key_of[2], (FF, K), FF ** -0.5, 0.03125, ((0, 4),))
    proj_out = centred(key_of[3], (D, K), D ** -0.5, 0.0625, ((0, 4),))
    validation = centred(key_of[4], (NVAL, SK), SK ** -0.5, 0.09375, ((0, 4), (1, 32)))
    doc_lengths = draw_doc_lengths(jax.random.fold_in(key_of[7], 71), 0)
    owner_rows = draw_owner_rows(jax.random.fold_in(key_of[7], 71), 0)
    return {"activations": activations, "out_grads": out_grads, "proj_in": proj_in, "proj_out": proj_out, "validation": validation, "doc_lengths": doc_lengths, "owner_rows": owner_rows}


def row_sketch(act_row, grad_row, lengths, proj_in, proj_out):
    act_proj = jnp.dot(act_row, proj_in, preferred_element_type=jnp.float32)
    grad_proj = jnp.dot(grad_row, proj_out, preferred_element_type=jnp.float32)
    tokens = act_proj.shape[0]
    outer_prod = (act_proj[:, :, None] * grad_proj[:, None, :]).reshape(tokens, -1)
    starts = (jnp.cumsum(lengths) - lengths).astype(jnp.int32)
    positions = jnp.arange(tokens, dtype=jnp.int32)
    member = ((positions[None, :] >= starts[:, None]) & (positions[None, :] < starts[:, None] + lengths[:, None])).astype(jnp.float32)
    summed = jnp.dot(member, outer_prod, precision=lax.Precision.HIGHEST, preferred_element_type=jnp.float32)
    scaling = 1.0 / jnp.sqrt(jnp.maximum(lengths, 1).astype(jnp.float32))
    return (summed * scaling[:, None]).astype(jnp.bfloat16)

def reference(activations, out_grads, proj_in, proj_out, validation, doc_lengths, owner_rows):
    act_rows = activations.reshape(N_DP, TOK_DEV, FF)
    grad_rows = out_grads.reshape(N_DP, TOK_DEV, D)
    sketches = lax.map(lambda items: row_sketch(items[0], items[1], items[2], proj_in, proj_out), (act_rows, grad_rows, doc_lengths))
    flat = sketches.reshape(N_DP * MAXDOC, K * K)
    local = jnp.dot(flat, validation.T, preferred_element_type=jnp.float32).astype(jnp.bfloat16)
    is_live = doc_lengths.reshape(-1) > 0
    local = jnp.where(is_live[:, None], local, jnp.zeros_like(local))
    result = jnp.zeros((N_DP * MAXDOC, NVAL), jnp.bfloat16)
    return result.at[owner_rows.reshape(-1)].set(local)
```

```python
import jax
import jax.numpy as jnp
from jax import lax
from jax.experimental import pallas as pl
from jax.experimental.pallas import tpu as pltpu
from jax.sharding import PartitionSpec as P

MESH = pl.DeviceIdType.MESH
F32 = jnp.float32
BF16 = jnp.bfloat16

CH = 128
NCH = 8
NRS = 6
LAG = 4
NT = 4
ND = 32
SUB = CH // NT
AHEAD = 3


def bytes_wait(ref, sem):
    pltpu.make_async_copy(ref, ref, sem).wait()


def kernel(
    act_hbm, grad_hbm, pin_hbm, pout_hbm, val_hbm, len_hbm, own_hbm, out_hbm,
    act_v, grad_v, pin_v, pout_v, len_v, own_v,
    part, rsbuf, dbuf, full, vbuf, params, lab_out, lab_in, sc_out, sc_in,
    at_ref, lhs_ref, s_ref, out_v,
    act_sem, grad_sem, misc_sem,
    v_send, v_recv, vf_send, vf_recv, rs_send, rs_recv, ag_send, ag_recv,
    lab_send, lab_recv, sc_send, sc_recv,
):
    r = lax.axis_index("dp")
    t = lax.axis_index("tensor")
    core = lax.rem(r, 2)
    chip = r // 2
    sibling = chip * 2 + (1 - core)

    def act_copy(c):
        rows = pl.ds(pl.multiple_of(c * CH, CH), CH)
        return pltpu.make_async_copy(act_hbm.at[rows], act_v.at[rows], act_sem.at[c])

    def grad_copy(c):
        rows = pl.ds(pl.multiple_of(c * CH, CH), CH)
        return pltpu.make_async_copy(grad_hbm.at[rows], grad_v.at[rows], grad_sem.at[c])

    pin_copy = pltpu.make_async_copy(pin_hbm, pin_v, misc_sem.at[0])
    pout_copy = pltpu.make_async_copy(pout_hbm, pout_v, misc_sem.at[1])
    val_copy = pltpu.make_async_copy(val_hbm, vbuf.at[r], misc_sem.at[2])
    len_copy = pltpu.make_async_copy(len_hbm, len_v, misc_sem.at[3])
    own_copy = pltpu.make_async_copy(own_hbm, own_v, misc_sem.at[4])

    len_copy.start()
    own_copy.start()
    pin_copy.start()
    act_copy(0).start()
    pout_copy.start()
    grad_copy(0).start()
    val_copy.start()
    for c in range(1, AHEAD):
        act_copy(c).start()
        grad_copy(c).start()

    barrier = pltpu.get_barrier_semaphore()

    def greet(i, carry):
        other = lax.rem(r + i, ND)
        pl.semaphore_signal(barrier, inc=1, device_id=(other, t), device_id_type=MESH)
        return carry

    lax.fori_loop(1, ND, greet, 0)
    for d in range(1, NT):
        pl.semaphore_signal(
            barrier, inc=1, device_id=(r, lax.rem(t + d, NT)), device_id_type=MESH
        )

    len_copy.wait()
    own_copy.wait()
    lens = len_v[...].astype(F32)
    rows_out = own_v[...]
    owner = rows_out // ND
    slot = (rows_out - owner * ND).astype(F32)
    row_id = lax.broadcasted_iota(jnp.int32, (ND, ND), 0)
    col_id = lax.broadcasted_iota(jnp.int32, (ND, ND), 1)
    chosen = jnp.broadcast_to(owner, (ND, ND)) == row_id
    zero = jnp.zeros((ND, ND), F32)
    doc_at = jnp.sum(jnp.where(chosen, col_id.astype(F32), zero), axis=1, keepdims=True)
    slot_at = jnp.sum(
        jnp.where(chosen, jnp.broadcast_to(slot, (ND, ND)), zero), axis=1, keepdims=True
    )
    lens_all = jnp.broadcast_to(lens, (ND, ND))
    len_at = jnp.sum(jnp.where(chosen, lens_all, zero), axis=1, keepdims=True)
    end_at = jnp.sum(
        jnp.where(col_id.astype(F32) <= doc_at, lens_all, zero), axis=1, keepdims=True
    )
    start_at = end_at - len_at
    params[0] = jnp.broadcast_to(start_at, (ND, 128))
    params[1] = jnp.broadcast_to(end_at, (ND, 128))
    params[2] = jnp.broadcast_to(1.0 / jnp.sqrt(jnp.maximum(len_at, 1.0)), (ND, 128))
    slots_wide = jnp.broadcast_to(slot_at, (ND, 128))
    for i in range(ND):
        lab_out[i] = slots_wide[i : i + 1, :]
    s_ref[...] = jnp.zeros_like(s_ref)

    def multiply(c):
        rows = pl.ds(pl.multiple_of(c * CH, CH), CH)
        act_copy(c).wait()
        left = jnp.dot(act_v[rows, :], pin_v[...], preferred_element_type=F32)
        grad_copy(c).wait()
        right = jnp.dot(grad_v[rows, :], pout_v[...], preferred_element_type=F32)
        part[c] = jnp.concatenate([left, right], axis=1).astype(BF16)

    def scatter_copy(c, d):
        peer = lax.rem(t + d, NT)
        return pltpu.make_async_remote_copy(
            src_ref=part.at[c, pl.ds(pl.multiple_of(peer * SUB, SUB), SUB)],
            dst_ref=rsbuf.at[c, d - 1],
            send_sem=rs_send.at[c],
            recv_sem=rs_recv.at[c],
            device_id=(r, peer),
            device_id_type=MESH,
        )

    def direct_copy(c, d):
        peer = lax.rem(t + d, NT)
        return pltpu.make_async_remote_copy(
            src_ref=part.at[c],
            dst_ref=dbuf.at[c - NRS, d - 1],
            send_sem=rs_send.at[c],
            recv_sem=rs_recv.at[c],
            device_id=(r, peer),
            device_id_type=MESH,
        )

    def gather_copy(c, d):
        peer = lax.rem(t + d, NT)
        mine = full.at[c, pl.ds(pl.multiple_of(t * SUB, SUB), SUB)]
        return pltpu.make_async_remote_copy(
            src_ref=mine,
            dst_ref=mine,
            send_sem=ag_send.at[c],
            recv_sem=ag_recv.at[c],
            device_id=(r, peer),
            device_id_type=MESH,
        )

    def reduce(c):
        bytes_wait(rsbuf.at[c], rs_recv.at[c])
        mine = pl.ds(pl.multiple_of(t * SUB, SUB), SUB)
        total = part[c, mine, :].astype(F32)
        for d in range(NT - 1):
            total = total + rsbuf[c, d].astype(F32)
        full[c, mine, :] = total.astype(BF16)
        for d in (2, 1, 3):
            gather_copy(c, d).start()

    pin_copy.wait()
    pout_copy.wait()
    multiply(0)
    pl.semaphore_wait(barrier, ND - 1 + NT - 1)
    for d in (2, 1, 3):
        scatter_copy(0, d).start()

    val_copy.wait()

    def val_to(peer, send, recv, block):
        return pltpu.make_async_remote_copy(
            src_ref=vbuf.at[block],
            dst_ref=vbuf.at[block],
            send_sem=send,
            recv_sem=recv,
            device_id=(peer, t),
            device_id_type=MESH,
        )

    def val_out(i, carry):
        peer = lax.rem(chip + i, ND // 2) * 2 + core
        val_to(peer, v_send, v_recv, r).start()
        return carry

    lax.fori_loop(1, ND // 2, val_out, 0)
    val_to(sibling, vf_send, vf_recv, r).start()

    def lab_copy(i):
        peer = lax.rem(r + i, ND)
        return pltpu.make_async_remote_copy(
            src_ref=lab_out.at[peer],
            dst_ref=lab_in.at[r],
            send_sem=lab_send,
            recv_sem=lab_recv,
            device_id=(peer, t),
            device_id_type=MESH,
        )

    def lab_go(i, carry):
        lab_copy(i).start()
        return carry

    lax.fori_loop(1, ND, lab_go, 0)
    lab_in[r] = lab_out[r]

    def step(c, carry):
        @pl.when(c + (AHEAD - 1) < NCH)
        def _():
            act_copy(c + (AHEAD - 1)).start()
            grad_copy(c + (AHEAD - 1)).start()

        multiply(c)

        @pl.when(c < NRS)
        def _():
            for d in (2, 1, 3):
                scatter_copy(c, d).start()

        @pl.when(c >= NRS)
        def _():
            for d in (2, 1, 3):
                direct_copy(c, d).start()

        @pl.when(c >= LAG)
        def _():
            reduce(c - LAG)

        return carry

    lax.fori_loop(1, NCH, step, 0)
    for c in range(NCH - LAG, NRS):
        reduce(c)

    bytes_wait(vbuf.at[pl.ds(0, ND // 2 - 1)], v_recv)

    def val_forward(i, carry):
        block = lax.rem(chip + i, ND // 2) * 2 + core
        val_to(sibling, vf_send, vf_recv, block).start()
        return carry

    lax.fori_loop(1, ND // 2, val_forward, 0)

    bytes_wait(lab_in.at[pl.ds(0, ND - 1)], lab_recv)
    slots_in = jnp.concatenate([lab_in[i] for i in range(ND)], axis=0)
    lane = lax.broadcasted_iota(jnp.int32, (ND, 128), 1).astype(F32)
    place = (slots_in == lane).astype(F32)

    lane_a = lax.broadcasted_iota(jnp.int32, (64, 128), 1)
    row_a = lax.broadcasted_iota(jnp.int32, (64, 128), 0)
    pick = jnp.where(row_a < 32, 2 * row_a, 2 * (row_a - 32) + 1)
    spread = (lane_a == pick).astype(BF16)
    low = lax.broadcasted_iota(jnp.int32, (CH, 128), 1) < 64

    def sketch(c, total):
        both = total.astype(BF16)
        turned = lax.dot_general(
            spread, both, (((1,), (1,)), ((), ())), preferred_element_type=F32
        )
        at_ref[:, 0:CH] = turned[0:32]
        at_ref[:, CH : 2 * CH] = turned[32:64]
        rolled = pltpu.roll(total, 64, 1)
        upper = jnp.where(low, rolled, 0.0).astype(BF16)
        lower = jnp.where(low, 0.0, total).astype(BF16)
        rhs = jnp.concatenate([upper, lower], axis=0)
        base = jnp.asarray(c * CH, F32)
        pos = lax.broadcasted_iota(jnp.int32, (ND, CH), 1).astype(F32) + base
        member = ((pos >= params[0]) & (pos < params[1])).astype(F32)
        member = jnp.concatenate([member, member], axis=1)
        for k in range(32):
            lhs_ref[k * ND : (k + 1) * ND, :] = (at_ref[k : k + 1, :] * member).astype(BF16)
        s_ref[...] += jnp.dot(lhs_ref[...], rhs, preferred_element_type=F32)

    def sketch_gathered(c, carry):
        bytes_wait(rsbuf.at[c], ag_recv.at[c])
        sketch(c, full[c].astype(F32))
        return carry

    lax.fori_loop(0, NRS, sketch_gathered, 0)

    def sketch_direct(c, carry):
        bytes_wait(dbuf.at[c - NRS], rs_recv.at[c])
        total = part[c].astype(F32)
        for d in range(NT - 1):
            total = total + dbuf[c - NRS, d].astype(F32)
        sketch(c, total)
        return carry

    lax.fori_loop(NRS, NCH, sketch_direct, 0)

    bytes_wait(vbuf.at[pl.ds(0, ND // 2)], vf_recv)
    local = jnp.zeros((ND, 128), F32)
    for k in range(0, 32, 2):
        left = jnp.concatenate(
            [s_ref[k * ND : (k + 1) * ND, :], s_ref[(k + 1) * ND : (k + 2) * ND, :]], axis=1
        ).astype(BF16)
        right = jnp.concatenate([vbuf[k], vbuf[k + 1]], axis=1)
        local = local + lax.dot_general(
            left, right, (((1,), (1,)), ((), ())), preferred_element_type=F32
        )
    local = local * params[2]
    for i in range(ND):
        sc_out[i] = local[i : i + 1, :]

    def score_copy(i):
        peer = lax.rem(r + i, ND)
        return pltpu.make_async_remote_copy(
            src_ref=sc_out.at[peer],
            dst_ref=sc_in.at[r],
            send_sem=sc_send,
            recv_sem=sc_recv,
            device_id=(peer, t),
            device_id_type=MESH,
        )

    def score_go(i, carry):
        score_copy(i).start()
        return carry

    lax.fori_loop(1, ND, score_go, 0)
    sc_in[r] = sc_out[r]

    for c in range(NRS):
        bytes_wait(rsbuf.at[c], rs_send.at[c])
        bytes_wait(rsbuf.at[c], ag_send.at[c])
    for c in range(NRS, NCH):
        bytes_wait(dbuf.at[c - NRS], rs_send.at[c])
    bytes_wait(vbuf.at[pl.ds(0, ND // 2 - 1)], v_send)
    bytes_wait(vbuf.at[pl.ds(0, ND // 2)], vf_send)
    bytes_wait(lab_out.at[pl.ds(0, ND - 1)], lab_send)

    bytes_wait(sc_in.at[pl.ds(0, ND - 1)], sc_recv)
    came = jnp.concatenate([sc_in[i] for i in range(ND)], axis=0)
    placed = lax.dot_general(
        place.astype(BF16),
        came.astype(BF16),
        (((0,), (0,)), ((), ())),
        preferred_element_type=F32,
    )
    out_v[...] = placed[0:ND].astype(BF16)
    out_copy = pltpu.make_async_copy(out_v, out_hbm, misc_sem.at[5])
    out_copy.start()
    bytes_wait(sc_out.at[pl.ds(0, ND - 1)], sc_send)
    out_copy.wait()


def shards(activations, out_grads, proj_in, proj_out, validation, doc_lengths, owner_rows):
    tokens, width_in = activations.shape
    width_out = out_grads.shape[1]
    dma = pltpu.SemaphoreType.DMA
    any_spec = pl.BlockSpec(memory_space=pl.ANY)
    return pl.pallas_call(
        kernel,
        out_shape=jax.ShapeDtypeStruct((ND, 128), BF16),
        in_specs=[any_spec] * 7,
        out_specs=any_spec,
        scratch_shapes=[
            pltpu.VMEM((tokens, width_in), BF16),
            pltpu.VMEM((tokens, width_out), BF16),
            pltpu.VMEM((width_in, 64), BF16),
            pltpu.VMEM((width_out, 64), BF16),
            pltpu.VMEM((1, ND), jnp.int32),
            pltpu.VMEM((1, ND), jnp.int32),
            pltpu.VMEM((NCH, CH, 128), BF16),
            pltpu.VMEM((NRS, NT - 1, SUB, 128), BF16),
            pltpu.VMEM((NCH - NRS, NT - 1, CH, 128), BF16),
            pltpu.VMEM((NRS, CH, 128), BF16),
            pltpu.VMEM((ND, 128, 128), BF16),
            pltpu.VMEM((3, ND, 128), F32),
            pltpu.VMEM((ND, 1, 128), F32),
            pltpu.VMEM((ND, 1, 128), F32),
            pltpu.VMEM((ND, 1, 128), F32),
            pltpu.VMEM((ND, 1, 128), F32),
            pltpu.VMEM((32, 2 * CH), F32),
            pltpu.VMEM((32 * ND, 2 * CH), BF16),
            pltpu.VMEM((32 * ND, 128), F32),
            pltpu.VMEM((ND, 128), BF16),
            dma((NCH,)),
            dma((NCH,)),
            dma((6,)),
            dma,
            dma,
            dma,
            dma,
            dma((NCH,)),
            dma((NCH,)),
            dma((NRS,)),
            dma((NRS,)),
            dma,
            dma,
            dma,
            dma,
        ],
        compiler_params=pltpu.CompilerParams(collective_id=0, has_side_effects=True),
        name="sketch_scores",
    )(activations, out_grads, proj_in, proj_out, validation, doc_lengths, owner_rows)


def solution(mesh):
    placed = (
        P("dp", "tensor"),
        P("dp", "tensor"),
        P("tensor", None),
        P("tensor", None),
        P("tensor", "dp"),
        P("dp", None),
        P("dp", None),
    )
    return jax.shard_map(
        shards, mesh=mesh, in_specs=placed, out_specs=P("dp", "tensor"), check_vma=False
    )
```

```python
import jax
import jax.numpy as jnp
from jax import lax
from jax.experimental import pallas as pl
from jax.experimental.pallas import tpu as pltpu
from jax.sharding import PartitionSpec as P

MESH = pl.DeviceIdType.MESH
F32 = jnp.float32
BF16 = jnp.bfloat16

NT_DIMS = (((1,), (1,)), ((), ()))
CH = 128
NCH = 8
NRS = 6
LAG = 4
NT = 4
ND = 32
SUB = CH // NT
AHEAD = 3


def bytes_wait(ref, sem):
    pltpu.make_async_copy(ref, ref, sem).wait()


def kernel(
    act_hbm, grad_hbm, pin_hbm, pout_hbm, val_hbm, len_hbm, own_hbm, out_hbm,
    act_v, grad_v, pin_v, pout_v, len_v, own_v,
    part, rsbuf, dbuf, full, vbuf, params, lab_out, lab_in, sc_out, sc_in,
    at_ref, lhs_ref, s_ref, out_v,
    act_sem, grad_sem, misc_sem,
    v_send, v_recv, vf_send, vf_recv, rs_send, rs_recv, ag_send, ag_recv,
    lab_send, lab_recv, sc_send, sc_recv,
):
    r = lax.axis_index("dp")
    t = lax.axis_index("tensor")
    core = lax.rem(r, 2)
    chip = r // 2
    sibling = chip * 2 + (1 - core)

    def act_copy(c):
        rows = pl.ds(pl.multiple_of(c * CH, CH), CH)
        return pltpu.make_async_copy(act_hbm.at[rows], act_v.at[rows], act_sem.at[c])

    def grad_copy(c):
        rows = pl.ds(pl.multiple_of(c * CH, CH), CH)
        return pltpu.make_async_copy(grad_hbm.at[rows], grad_v.at[rows], grad_sem.at[c])

    pin_copy = pltpu.make_async_copy(pin_hbm, pin_v, misc_sem.at[0])
    pout_copy = pltpu.make_async_copy(pout_hbm, pout_v, misc_sem.at[1])
    val_copy = pltpu.make_async_copy(val_hbm, vbuf.at[r], misc_sem.at[2])
    len_copy = pltpu.make_async_copy(len_hbm, len_v, misc_sem.at[3])
    own_copy = pltpu.make_async_copy(own_hbm, own_v, misc_sem.at[4])

    len_copy.start()
    own_copy.start()
    pin_copy.start()
    act_copy(0).start()
    pout_copy.start()
    grad_copy(0).start()
    val_copy.start()
    for c in range(1, AHEAD):
        act_copy(c).start()
        grad_copy(c).start()

    barrier = pltpu.get_barrier_semaphore()

    def greet(i, carry):
        other = lax.rem(r + i, ND)
        pl.semaphore_signal(barrier, inc=1, device_id=(other, t), device_id_type=MESH)
        return carry

    lax.fori_loop(1, ND, greet, 0)
    for d in range(1, NT):
        pl.semaphore_signal(
            barrier, inc=1, device_id=(r, lax.rem(t + d, NT)), device_id_type=MESH
        )

    len_copy.wait()
    own_copy.wait()
    lens = len_v[...].astype(F32)
    rows_out = own_v[...]
    owner = rows_out // ND
    slot = (rows_out - owner * ND).astype(F32)
    row_id = lax.broadcasted_iota(jnp.int32, (ND, ND), 0)
    col_id = lax.broadcasted_iota(jnp.int32, (ND, ND), 1)
    chosen = jnp.broadcast_to(owner, (ND, ND)) == row_id
    zero = jnp.zeros((ND, ND), F32)
    doc_at = jnp.sum(jnp.where(chosen, col_id.astype(F32), zero), axis=1, keepdims=True)
    slot_at = jnp.sum(
        jnp.where(chosen, jnp.broadcast_to(slot, (ND, ND)), zero), axis=1, keepdims=True
    )
    lens_all = jnp.broadcast_to(lens, (ND, ND))
    len_at = jnp.sum(jnp.where(chosen, lens_all, zero), axis=1, keepdims=True)
    end_at = jnp.sum(
        jnp.where(col_id.astype(F32) <= doc_at, lens_all, zero), axis=1, keepdims=True
    )
    start_at = end_at - len_at
    params[0] = jnp.broadcast_to(start_at, (ND, 128))
    params[1] = jnp.broadcast_to(end_at, (ND, 128))
    params[2] = jnp.broadcast_to(1.0 / jnp.sqrt(jnp.maximum(len_at, 1.0)), (ND, 128))
    slots_wide = jnp.broadcast_to(slot_at, (ND, 128))
    for i in range(ND):
        lab_out[i] = slots_wide[i : i + 1, :]
    s_ref[...] = jnp.zeros_like(s_ref)

    def multiply(c):
        rows = pl.ds(pl.multiple_of(c * CH, CH), CH)
        act_copy(c).wait()
        grad_copy(c).wait()
        left = lax.dot_general(act_v[rows, :], pin_v[...], NT_DIMS, preferred_element_type=F32)
        right = lax.dot_general(grad_v[rows, :], pout_v[...], NT_DIMS, preferred_element_type=F32)
        part[c] = jnp.concatenate([left, right], axis=1).astype(BF16)

    def scatter_copy(c, d):
        peer = lax.rem(t + d, NT)
        return pltpu.make_async_remote_copy(
            src_ref=part.at[c, pl.ds(pl.multiple_of(peer * SUB, SUB), SUB)],
            dst_ref=rsbuf.at[c, d - 1],
            send_sem=rs_send.at[c],
            recv_sem=rs_recv.at[c],
            device_id=(r, peer),
            device_id_type=MESH,
        )

    def direct_copy(c, d):
        peer = lax.rem(t + d, NT)
        return pltpu.make_async_remote_copy(
            src_ref=part.at[c],
            dst_ref=dbuf.at[c - NRS, d - 1],
            send_sem=rs_send.at[c],
            recv_sem=rs_recv.at[c],
            device_id=(r, peer),
            device_id_type=MESH,
        )

    def gather_copy(c, d):
        peer = lax.rem(t + d, NT)
        mine = full.at[c, pl.ds(pl.multiple_of(t * SUB, SUB), SUB)]
        return pltpu.make_async_remote_copy(
            src_ref=mine,
            dst_ref=mine,
            send_sem=ag_send.at[c],
            recv_sem=ag_recv.at[c],
            device_id=(r, peer),
            device_id_type=MESH,
        )

    def reduce(c):
        bytes_wait(rsbuf.at[c], rs_recv.at[c])
        mine = pl.ds(pl.multiple_of(t * SUB, SUB), SUB)
        total = part[c, mine, :].astype(F32)
        for d in range(NT - 1):
            total = total + rsbuf[c, d].astype(F32)
        full[c, mine, :] = total.astype(BF16)
        for d in (2, 1, 3):
            gather_copy(c, d).start()

    pin_copy.wait()
    pout_copy.wait()
    multiply(0)
    pl.semaphore_wait(barrier, ND - 1 + NT - 1)
    for d in (2, 1, 3):
        scatter_copy(0, d).start()

    val_copy.wait()

    def val_to(peer, send, recv, block):
        return pltpu.make_async_remote_copy(
            src_ref=vbuf.at[block],
            dst_ref=vbuf.at[block],
            send_sem=send,
            recv_sem=recv,
            device_id=(peer, t),
            device_id_type=MESH,
        )

    def val_out(i, carry):
        peer = lax.rem(chip + i, ND // 2) * 2 + core
        val_to(peer, v_send, v_recv, r).start()
        return carry

    lax.fori_loop(1, ND // 2, val_out, 0)
    val_to(sibling, vf_send, vf_recv, r).start()

    def lab_copy(i):
        peer = lax.rem(r + i, ND)
        return pltpu.make_async_remote_copy(
            src_ref=lab_out.at[peer],
            dst_ref=lab_in.at[r],
            send_sem=lab_send,
            recv_sem=lab_recv,
            device_id=(peer, t),
            device_id_type=MESH,
        )

    def lab_go(i, carry):
        lab_copy(i).start()
        return carry

    lax.fori_loop(1, ND, lab_go, 0)
    lab_in[r] = lab_out[r]

    def step(c, carry):
        @pl.when(c + (AHEAD - 1) < NCH)
        def _():
            act_copy(c + (AHEAD - 1)).start()
            grad_copy(c + (AHEAD - 1)).start()

        multiply(c)

        @pl.when(c < NRS)
        def _():
            for d in (2, 1, 3):
                scatter_copy(c, d).start()

        @pl.when(c >= NRS)
        def _():
            for d in (2, 1, 3):
                direct_copy(c, d).start()

        @pl.when(c >= LAG)
        def _():
            reduce(c - LAG)

        return carry

    lax.fori_loop(1, NCH, step, 0)
    for c in range(NCH - LAG, NRS):
        reduce(c)

    bytes_wait(vbuf.at[pl.ds(0, ND // 2 - 1)], v_recv)

    def val_forward(i, carry):
        block = lax.rem(chip + i, ND // 2) * 2 + core
        val_to(sibling, vf_send, vf_recv, block).start()
        return carry

    lax.fori_loop(1, ND // 2, val_forward, 0)

    bytes_wait(lab_in.at[pl.ds(0, ND - 1)], lab_recv)
    slots_in = jnp.concatenate([lab_in[i] for i in range(ND)], axis=0)
    lane = lax.broadcasted_iota(jnp.int32, (ND, 128), 1).astype(F32)
    place = (slots_in == lane).astype(BF16)
    eye = (row_id == col_id).astype(BF16)
    place = lax.dot_general(
        place, eye, (((0,), (0,)), ((), ())), preferred_element_type=F32
    )[0:ND].astype(BF16)

    lane_a = lax.broadcasted_iota(jnp.int32, (64, 128), 1)
    row_a = lax.broadcasted_iota(jnp.int32, (64, 128), 0)
    pick = jnp.where(row_a < 32, 2 * row_a, 2 * (row_a - 32) + 1)
    spread = (lane_a == pick).astype(BF16)
    low = lax.broadcasted_iota(jnp.int32, (CH, 128), 1) < 64

    def sketch(c, total):
        both = total.astype(BF16)
        turned = lax.dot_general(
            spread, both, (((1,), (1,)), ((), ())), preferred_element_type=F32
        )
        at_ref[:, 0:CH] = turned[0:32]
        at_ref[:, CH : 2 * CH] = turned[32:64]
        rolled = pltpu.roll(total, 64, 1)
        upper = jnp.where(low, rolled, 0.0).astype(BF16)
        lower = jnp.where(low, 0.0, total).astype(BF16)
        rhs = jnp.concatenate([upper, lower], axis=0)
        base = jnp.asarray(c * CH, F32)
        pos = lax.broadcasted_iota(jnp.int32, (ND, CH), 1).astype(F32) + base
        member = ((pos >= params[0]) & (pos < params[1])).astype(F32)
        member = jnp.concatenate([member, member], axis=1)
        for k in range(32):
            lhs_ref[k * ND : (k + 1) * ND, :] = (at_ref[k : k + 1, :] * member).astype(BF16)
        s_ref[...] += jnp.dot(lhs_ref[...], rhs, preferred_element_type=F32)

    def sketch_gathered(c, carry):
        bytes_wait(rsbuf.at[c], ag_recv.at[c])
        sketch(c, full[c].astype(F32))
        return carry

    lax.fori_loop(0, NRS, sketch_gathered, 0)

    def sketch_direct(c, carry):
        bytes_wait(dbuf.at[c - NRS], rs_recv.at[c])
        total = part[c].astype(F32)
        for d in range(NT - 1):
            total = total + dbuf[c - NRS, d].astype(F32)
        sketch(c, total)
        return carry

    lax.fori_loop(NRS, NCH, sketch_direct, 0)

    bytes_wait(vbuf.at[pl.ds(0, ND // 2)], vf_recv)
    local = jnp.zeros((ND, 128), F32)
    for k in range(0, 32, 2):
        left = jnp.concatenate(
            [s_ref[k * ND : (k + 1) * ND, :], s_ref[(k + 1) * ND : (k + 2) * ND, :]], axis=1
        ).astype(BF16)
        right = jnp.concatenate([vbuf[k], vbuf[k + 1]], axis=1)
        local = local + lax.dot_general(
            left, right, (((1,), (1,)), ((), ())), preferred_element_type=F32
        )
    local = local * params[2]
    for i in range(ND):
        sc_out[i] = local[i : i + 1, :]

    def score_copy(i):
        peer = lax.rem(r + i, ND)
        return pltpu.make_async_remote_copy(
            src_ref=sc_out.at[peer],
            dst_ref=sc_in.at[r],
            send_sem=sc_send,
            recv_sem=sc_recv,
            device_id=(peer, t),
            device_id_type=MESH,
        )

    def score_go(i, carry):
        score_copy(i).start()
        return carry

    lax.fori_loop(1, ND, score_go, 0)
    sc_in[r] = sc_out[r]

    for c in range(NRS):
        bytes_wait(rsbuf.at[c], rs_send.at[c])
        bytes_wait(rsbuf.at[c], ag_send.at[c])
    for c in range(NRS, NCH):
        bytes_wait(dbuf.at[c - NRS], rs_send.at[c])
    bytes_wait(vbuf.at[pl.ds(0, ND // 2 - 1)], v_send)
    bytes_wait(vbuf.at[pl.ds(0, ND // 2)], vf_send)
    bytes_wait(lab_out.at[pl.ds(0, ND - 1)], lab_send)

    bytes_wait(sc_in.at[pl.ds(0, ND - 1)], sc_recv)
    came = jnp.concatenate([sc_in[i] for i in range(ND)], axis=0)
    placed = jnp.dot(place, came.astype(BF16), preferred_element_type=F32)
    out_v[...] = placed.astype(BF16)
    out_copy = pltpu.make_async_copy(out_v, out_hbm, misc_sem.at[5])
    out_copy.start()
    bytes_wait(sc_out.at[pl.ds(0, ND - 1)], sc_send)
    out_copy.wait()


def shards(activations, out_grads, proj_in, proj_out, validation, doc_lengths, owner_rows):
    tokens, width_in = activations.shape
    width_out = out_grads.shape[1]
    dma = pltpu.SemaphoreType.DMA
    any_spec = pl.BlockSpec(memory_space=pl.ANY)
    return pl.pallas_call(
        kernel,
        out_shape=jax.ShapeDtypeStruct((ND, 128), BF16),
        in_specs=[any_spec] * 7,
        out_specs=any_spec,
        scratch_shapes=[
            pltpu.VMEM((tokens, width_in), BF16),
            pltpu.VMEM((tokens, width_out), BF16),
            pltpu.VMEM((64, width_in), BF16),
            pltpu.VMEM((64, width_out), BF16),
            pltpu.VMEM((1, ND), jnp.int32),
            pltpu.VMEM((1, ND), jnp.int32),
            pltpu.VMEM((NCH, CH, 128), BF16),
            pltpu.VMEM((NRS, NT - 1, SUB, 128), BF16),
            pltpu.VMEM((NCH - NRS, NT - 1, CH, 128), BF16),
            pltpu.VMEM((NRS, CH, 128), BF16),
            pltpu.VMEM((ND, 128, 128), BF16),
            pltpu.VMEM((3, ND, 128), F32),
            pltpu.VMEM((ND, 1, 128), F32),
            pltpu.VMEM((ND, 1, 128), F32),
            pltpu.VMEM((ND, 1, 128), F32),
            pltpu.VMEM((ND, 1, 128), F32),
            pltpu.VMEM((32, 2 * CH), F32),
            pltpu.VMEM((32 * ND, 2 * CH), BF16),
            pltpu.VMEM((32 * ND, 128), F32),
            pltpu.VMEM((ND, 128), BF16),
            dma((NCH,)),
            dma((NCH,)),
            dma((6,)),
            dma,
            dma,
            dma,
            dma,
            dma((NCH,)),
            dma((NCH,)),
            dma((NRS,)),
            dma((NRS,)),
            dma,
            dma,
            dma,
            dma,
        ],
        compiler_params=pltpu.CompilerParams(collective_id=0, has_side_effects=True),
        name="sketch_scores",
    )(activations, out_grads, proj_in.T, proj_out.T, validation, doc_lengths, owner_rows)


def solution(mesh):
    placed = (
        P("dp", "tensor"),
        P("dp", "tensor"),
        P("tensor", None),
        P("tensor", None),
        P("tensor", "dp"),
        P("dp", None),
        P("dp", None),
    )
    return jax.shard_map(
        shards, mesh=mesh, in_specs=placed, out_specs=P("dp", "tensor"), check_vma=False
    )
```

```python
import jax
import jax.numpy as jnp
from jax import lax
from jax.experimental import pallas as pl
from jax.experimental.pallas import tpu as pltpu
from jax.sharding import PartitionSpec as P

MESH = pl.DeviceIdType.MESH
F32 = jnp.float32
BF16 = jnp.bfloat16

NT_DIMS = (((1,), (1,)), ((), ()))
CH = 128
NCH = 8
NRS = 6
LAG = 4
SECOND = 5
EARLY = 2
MIDDLE = 2
PAIR = 2 * CH
NT = 4
ND = 32
SUB = CH // NT
AHEAD = 3


def bytes_wait(ref, sem):
    pltpu.make_async_copy(ref, ref, sem).wait()


def kernel(
    act_hbm, grad_hbm, pin_hbm, pout_hbm, val_hbm, len_hbm, own_hbm, out_hbm,
    act_v, grad_v, pin_v, pout_v, len_v, own_v,
    part, rsbuf, dbuf, full, vbuf, params, lab_out, lab_in, sc_out, sc_in,
    at_ref, lhs_ref, s_ref, out_v,
    act_sem, grad_sem, misc_sem,
    v_send, v_recv, rs_send, rs_recv, ag_send, ag_recv,
    lab_send, lab_recv, sc_send, sc_recv,
):
    r = lax.axis_index("dp")
    t = lax.axis_index("tensor")
    core = lax.rem(r, 2)
    chip = r // 2
    x = lax.rem(chip, 4)
    y = chip // 4
    sibling = chip * 2 + (1 - core)

    def act_copy(c):
        rows = pl.ds(pl.multiple_of(c * CH, CH), CH)
        return pltpu.make_async_copy(act_hbm.at[rows], act_v.at[rows], act_sem.at[c])

    def grad_copy(c):
        rows = pl.ds(pl.multiple_of(c * CH, CH), CH)
        return pltpu.make_async_copy(grad_hbm.at[rows], grad_v.at[rows], grad_sem.at[c])

    pin_copy = pltpu.make_async_copy(pin_hbm, pin_v, misc_sem.at[0])
    pout_copy = pltpu.make_async_copy(pout_hbm, pout_v, misc_sem.at[1])
    val_a_copy = pltpu.make_async_copy(
        val_hbm.at[pl.ds(0, 64)], vbuf.at[core, 0, y, x], misc_sem.at[2]
    )
    val_b_copy = pltpu.make_async_copy(
        val_hbm.at[pl.ds(64, 64)], vbuf.at[core, 1, x, y], misc_sem.at[6]
    )
    len_copy = pltpu.make_async_copy(len_hbm, len_v, misc_sem.at[3])
    own_copy = pltpu.make_async_copy(own_hbm, own_v, misc_sem.at[4])

    len_copy.start()
    own_copy.start()
    pin_copy.start()
    act_copy(0).start()
    pout_copy.start()
    grad_copy(0).start()
    val_a_copy.start()
    val_b_copy.start()
    for c in range(1, AHEAD):
        act_copy(c).start()
        grad_copy(c).start()

    barrier = pltpu.get_barrier_semaphore()

    def greet(i, carry):
        other = lax.rem(r + i, ND)
        pl.semaphore_signal(barrier, inc=1, device_id=(other, t), device_id_type=MESH)
        return carry

    lax.fori_loop(1, ND, greet, 0)
    for d in range(1, NT):
        pl.semaphore_signal(
            barrier, inc=1, device_id=(r, lax.rem(t + d, NT)), device_id_type=MESH
        )

    len_copy.wait()
    own_copy.wait()
    lens = len_v[...].astype(F32)
    rows_out = own_v[...]
    owner = rows_out // ND
    slot = (rows_out - owner * ND).astype(F32)
    row_id = lax.broadcasted_iota(jnp.int32, (ND, ND), 0)
    col_id = lax.broadcasted_iota(jnp.int32, (ND, ND), 1)
    chosen = jnp.broadcast_to(owner, (ND, ND)) == row_id
    zero = jnp.zeros((ND, ND), F32)
    doc_at = jnp.sum(jnp.where(chosen, col_id.astype(F32), zero), axis=1, keepdims=True)
    slot_at = jnp.sum(
        jnp.where(chosen, jnp.broadcast_to(slot, (ND, ND)), zero), axis=1, keepdims=True
    )
    lens_all = jnp.broadcast_to(lens, (ND, ND))
    len_at = jnp.sum(jnp.where(chosen, lens_all, zero), axis=1, keepdims=True)
    end_at = jnp.sum(
        jnp.where(col_id.astype(F32) <= doc_at, lens_all, zero), axis=1, keepdims=True
    )
    start_at = end_at - len_at
    params[0] = jnp.broadcast_to(start_at, (ND, 128))
    params[1] = jnp.broadcast_to(end_at, (ND, 128))
    params[2] = jnp.broadcast_to(1.0 / jnp.sqrt(jnp.maximum(len_at, 1.0)), (ND, 128))
    slots_wide = jnp.broadcast_to(slot_at, (ND, 128))
    for i in range(ND):
        lab_out[i] = slots_wide[i : i + 1, :]
    s_ref[...] = jnp.zeros_like(s_ref)

    def multiply(c):
        rows = pl.ds(pl.multiple_of(c * CH, CH), CH)
        act_copy(c).wait()
        grad_copy(c).wait()
        left = lax.dot_general(act_v[rows, :], pin_v[...], NT_DIMS, preferred_element_type=F32)
        right = lax.dot_general(grad_v[rows, :], pout_v[...], NT_DIMS, preferred_element_type=F32)
        part[c] = jnp.concatenate([left, right], axis=1).astype(BF16)

    def scatter_copy(c, d):
        peer = lax.rem(t + d, NT)
        return pltpu.make_async_remote_copy(
            src_ref=part.at[c, pl.ds(pl.multiple_of(peer * SUB, SUB), SUB)],
            dst_ref=rsbuf.at[c, d - 1],
            send_sem=rs_send.at[c],
            recv_sem=rs_recv.at[c],
            device_id=(r, peer),
            device_id_type=MESH,
        )

    def direct_copy(c, d):
        peer = lax.rem(t + d, NT)
        return pltpu.make_async_remote_copy(
            src_ref=part.at[c],
            dst_ref=dbuf.at[c - NRS, d - 1],
            send_sem=rs_send.at[c],
            recv_sem=rs_recv.at[c],
            device_id=(r, peer),
            device_id_type=MESH,
        )

    def gather_copy(c, d):
        peer = lax.rem(t + d, NT)
        mine = full.at[c, pl.ds(pl.multiple_of(t * SUB, SUB), SUB)]
        return pltpu.make_async_remote_copy(
            src_ref=mine,
            dst_ref=mine,
            send_sem=ag_send.at[c],
            recv_sem=ag_recv.at[c],
            device_id=(r, peer),
            device_id_type=MESH,
        )

    def reduce(c):
        bytes_wait(rsbuf.at[c], rs_recv.at[c])
        mine = pl.ds(pl.multiple_of(t * SUB, SUB), SUB)
        total = part[c, mine, :].astype(F32)
        for d in range(NT - 1):
            total = total + rsbuf[c, d].astype(F32)
        full[c, mine, :] = total.astype(BF16)
        for d in (2, 1, 3):
            gather_copy(c, d).start()

    def ahead(c):
        @pl.when(c + (AHEAD - 1) < NCH)
        def _():
            act_copy(c + (AHEAD - 1)).start()
            grad_copy(c + (AHEAD - 1)).start()

    def early(c, carry):
        @pl.when(c > 0)
        def _():
            ahead(c)

        multiply(c)
        return carry

    pin_copy.wait()
    pout_copy.wait()
    lax.fori_loop(0, EARLY, early, 0)
    val_a_copy.wait()
    val_b_copy.wait()
    pl.semaphore_wait(barrier, ND - 1 + NT - 1)
    for d in (2, 1, 3):
        for c in range(EARLY):
            scatter_copy(c, d).start()

    def val_to(peer, send, recv, ref):
        return pltpu.make_async_remote_copy(
            src_ref=ref,
            dst_ref=ref,
            send_sem=send,
            recv_sem=recv,
            device_id=(peer, t),
            device_id_type=MESH,
        )

    def along_x(d):
        return (y * 4 + lax.rem(x + d, 4)) * 2 + core

    def along_y(d):
        return (lax.rem(y + d, 4) * 4 + x) * 2 + core

    for d in (2, 1, 3):
        val_to(along_x(d), v_send.at[0], v_recv.at[0], vbuf.at[core, 0, y, x]).start()
        val_to(along_y(d), v_send.at[1], v_recv.at[1], vbuf.at[core, 1, x, y]).start()

    def lab_copy(i):
        peer = lax.rem(r + i, ND)
        return pltpu.make_async_remote_copy(
            src_ref=lab_out.at[peer],
            dst_ref=lab_in.at[r],
            send_sem=lab_send,
            recv_sem=lab_recv,
            device_id=(peer, t),
            device_id_type=MESH,
        )

    def lab_go(i, carry):
        lab_copy(i).start()
        return carry

    lax.fori_loop(1, ND, lab_go, 0)
    lab_in[r] = lab_out[r]

    def val_second():
        bytes_wait(vbuf.at[0, 0, 0, pl.ds(0, 3)], v_recv.at[0])
        bytes_wait(vbuf.at[0, 0, 0, pl.ds(0, 3)], v_recv.at[1])
        for d in (2, 1, 3):
            val_to(along_y(d), v_send.at[2], v_recv.at[2], vbuf.at[core, 0, y]).start()
            val_to(along_x(d), v_send.at[3], v_recv.at[3], vbuf.at[core, 1, x]).start()

    def step(c, carry):
        ahead(c)
        multiply(c)

        @pl.when(c < NRS)
        def _():
            for d in (2, 1, 3):
                scatter_copy(c, d).start()

        @pl.when(c >= NRS)
        def _():
            for d in (2, 1, 3):
                direct_copy(c, d).start()

        @pl.when(c >= LAG)
        def _():
            reduce(c - LAG)

        @pl.when(c == SECOND)
        def _():
            val_second()

        return carry

    lax.fori_loop(EARLY, NCH, step, 0)
    for c in range(NCH - LAG, NRS):
        reduce(c)

    bytes_wait(lab_in.at[pl.ds(0, ND - 1)], lab_recv)
    slots_in = jnp.concatenate([lab_in[i] for i in range(ND)], axis=0)
    lane = lax.broadcasted_iota(jnp.int32, (ND, 128), 1).astype(F32)
    place = (slots_in == lane).astype(BF16)
    eye = (row_id == col_id).astype(BF16)
    place = lax.dot_general(
        place, eye, (((0,), (0,)), ((), ())), preferred_element_type=F32
    )[0:ND].astype(BF16)

    lane_a = lax.broadcasted_iota(jnp.int32, (64, 128), 1)
    row_a = lax.broadcasted_iota(jnp.int32, (64, 128), 0)
    pick = jnp.where(row_a < 32, 2 * row_a, 2 * (row_a - 32) + 1)
    spread = (lane_a == pick).astype(BF16)
    low = lax.broadcasted_iota(jnp.int32, (PAIR, 128), 1) < 64

    def sketch(p, total):
        turned = lax.dot_general(
            spread, total.astype(BF16), NT_DIMS, preferred_element_type=F32
        )
        at_ref[:, 0:PAIR] = turned[0:32]
        at_ref[:, PAIR : 2 * PAIR] = turned[32:64]
        rolled = pltpu.roll(total, 64, 1)
        upper = jnp.where(low, rolled, 0.0).astype(BF16)
        lower = jnp.where(low, 0.0, total).astype(BF16)
        rhs = jnp.concatenate([upper, lower], axis=0)
        pos = lax.broadcasted_iota(jnp.int32, (ND, 128), 1).astype(F32)
        pieces = []
        for i in range(PAIR // 128):
            at = pos + jnp.asarray(p * PAIR + i * 128, F32)
            pieces.append(((at >= params[0]) & (at < params[1])).astype(F32))
        member = jnp.concatenate(pieces + pieces, axis=1)
        for k in range(32):
            lhs_ref[k * ND : (k + 1) * ND, :] = (at_ref[k : k + 1, :] * member).astype(BF16)
        s_ref[...] += jnp.dot(lhs_ref[...], rhs, preferred_element_type=F32)

    def sketch_gathered(p, carry):
        for c in (2 * p, 2 * p + 1):
            bytes_wait(rsbuf.at[c], ag_recv.at[c])
        total = jnp.concatenate([full[2 * p], full[2 * p + 1]], axis=0)
        sketch(p, total.astype(F32))
        return carry

    lax.fori_loop(0, MIDDLE, sketch_gathered, 0)

    bytes_wait(vbuf.at[0, 0, pl.ds(0, 3)], v_recv.at[2])
    bytes_wait(vbuf.at[0, 0, pl.ds(0, 3)], v_recv.at[3])
    val_to(sibling, v_send.at[4], v_recv.at[4], vbuf.at[core]).start()

    lax.fori_loop(MIDDLE, NRS // 2, sketch_gathered, 0)

    def direct_total(c):
        bytes_wait(dbuf.at[c - NRS], rs_recv.at[c])
        total = part[c].astype(F32)
        for d in range(NT - 1):
            total = total + dbuf[c - NRS, d].astype(F32)
        return total

    def sketch_direct(p, carry):
        sketch(p, jnp.concatenate([direct_total(2 * p), direct_total(2 * p + 1)], axis=0))
        return carry

    lax.fori_loop(NRS // 2, NCH // 2, sketch_direct, 0)

    bytes_wait(vbuf.at[0], v_recv.at[4])
    local = jnp.zeros((ND, 128), F32)
    for k in range(0, 32, 2):
        left = jnp.concatenate(
            [s_ref[k * ND : (k + 1) * ND, :], s_ref[(k + 1) * ND : (k + 2) * ND, :]], axis=1
        ).astype(BF16)
        ky, kx = k // 8, (k // 2) % 4
        right = jnp.concatenate(
            [
                jnp.concatenate([vbuf[j, 0, ky, kx], vbuf[j, 1, kx, ky]], axis=0)
                for j in range(2)
            ],
            axis=1,
        )
        local = local + lax.dot_general(
            left, right, (((1,), (1,)), ((), ())), preferred_element_type=F32
        )
    local = local * params[2]
    for i in range(ND):
        sc_out[i] = local[i : i + 1, :]

    def score_copy(i):
        peer = lax.rem(r + i, ND)
        return pltpu.make_async_remote_copy(
            src_ref=sc_out.at[peer],
            dst_ref=sc_in.at[r],
            send_sem=sc_send,
            recv_sem=sc_recv,
            device_id=(peer, t),
            device_id_type=MESH,
        )

    def score_go(i, carry):
        score_copy(i).start()
        return carry

    lax.fori_loop(1, ND, score_go, 0)
    sc_in[r] = sc_out[r]

    for c in range(NRS):
        bytes_wait(rsbuf.at[c], rs_send.at[c])
        bytes_wait(rsbuf.at[c], ag_send.at[c])
    for c in range(NRS, NCH):
        bytes_wait(dbuf.at[c - NRS], rs_send.at[c])
    for i in range(2):
        bytes_wait(vbuf.at[0, 0, 0, pl.ds(0, 3)], v_send.at[i])
        bytes_wait(vbuf.at[0, 0, pl.ds(0, 3)], v_send.at[2 + i])
    bytes_wait(vbuf.at[0], v_send.at[4])
    bytes_wait(lab_out.at[pl.ds(0, ND - 1)], lab_send)

    bytes_wait(sc_in.at[pl.ds(0, ND - 1)], sc_recv)
    came = jnp.concatenate([sc_in[i] for i in range(ND)], axis=0)
    placed = jnp.dot(place, came.astype(BF16), preferred_element_type=F32)
    out_v[...] = placed.astype(BF16)
    out_copy = pltpu.make_async_copy(out_v, out_hbm, misc_sem.at[5])
    out_copy.start()
    bytes_wait(sc_out.at[pl.ds(0, ND - 1)], sc_send)
    out_copy.wait()


def shards(activations, out_grads, proj_in, proj_out, validation, doc_lengths, owner_rows):
    tokens, width_in = activations.shape
    width_out = out_grads.shape[1]
    dma = pltpu.SemaphoreType.DMA
    any_spec = pl.BlockSpec(memory_space=pl.ANY)
    return pl.pallas_call(
        kernel,
        out_shape=jax.ShapeDtypeStruct((ND, 128), BF16),
        in_specs=[any_spec] * 7,
        out_specs=any_spec,
        scratch_shapes=[
            pltpu.VMEM((tokens, width_in), BF16),
            pltpu.VMEM((tokens, width_out), BF16),
            pltpu.VMEM((64, width_in), BF16),
            pltpu.VMEM((64, width_out), BF16),
            pltpu.VMEM((1, ND), jnp.int32),
            pltpu.VMEM((1, ND), jnp.int32),
            pltpu.VMEM((NCH, CH, 128), BF16),
            pltpu.VMEM((NRS, NT - 1, SUB, 128), BF16),
            pltpu.VMEM((NCH - NRS, NT - 1, CH, 128), BF16),
            pltpu.VMEM((NRS, CH, 128), BF16),
            pltpu.VMEM((2, 2, 4, 4, 64, 128), BF16),
            pltpu.VMEM((3, ND, 128), F32),
            pltpu.VMEM((ND, 1, 128), F32),
            pltpu.VMEM((ND, 1, 128), F32),
            pltpu.VMEM((ND, 1, 128), F32),
            pltpu.VMEM((ND, 1, 128), F32),
            pltpu.VMEM((32, 2 * PAIR), F32),
            pltpu.VMEM((32 * ND, 2 * PAIR), BF16),
            pltpu.VMEM((32 * ND, 128), F32),
            pltpu.VMEM((ND, 128), BF16),
            dma((NCH,)),
            dma((NCH,)),
            dma((7,)),
            dma((5,)),
            dma((5,)),
            dma((NCH,)),
            dma((NCH,)),
            dma((NRS,)),
            dma((NRS,)),
            dma,
            dma,
            dma,
            dma,
        ],
        compiler_params=pltpu.CompilerParams(collective_id=0, has_side_effects=True),
        name="sketch_scores",
    )(activations, out_grads, proj_in.T, proj_out.T, validation, doc_lengths, owner_rows)


def solution(mesh):
    placed = (
        P("dp", "tensor"),
        P("dp", "tensor"),
        P("tensor", None),
        P("tensor", None),
        P("tensor", "dp"),
        P("dp", None),
        P("dp", None),
    )
    return jax.shard_map(
        shards, mesh=mesh, in_specs=placed, out_specs=P("dp", "tensor"), check_vma=False
    )
```

```python
import jax
import jax.numpy as jnp
from jax import lax
from jax.experimental import pallas as pl
from jax.experimental.pallas import tpu as pltpu
from jax.sharding import PartitionSpec as P

MESH = pl.DeviceIdType.MESH
F32 = jnp.float32
BF16 = jnp.bfloat16

NT_DIMS = (((1,), (1,)), ((), ()))
CH = 128
NCH = 1024 // CH
NRS = 7
LAG = 4
SECOND = 4
EARLY = 2
MIDDLE = 2
TOKENS_ROW = 1024
PAIR = 256
NT = 4
ND = 32
SUB = CH // NT
AHEAD = 3


def bytes_wait(ref, sem):
    pltpu.make_async_copy(ref, ref, sem).wait()


def kernel(
    act_hbm, grad_hbm, pin_hbm, pout_hbm, val_hbm, len_hbm, own_hbm, got_hbm, place_hbm,
    act_v, grad_v, pin_v, pout_v, len_v, own_v,
    part, rsbuf, dbuf, full, vbuf, params, lab_out, lab_in, sc_out,
    at_ref, lhs_ref, s_ref, place_v,
    act_sem, grad_sem, misc_sem,
    v_send, v_recv, rs_send, rs_recv, ag_send, ag_recv,
    lab_send, lab_recv, sc_send, sc_recv,
):
    r = lax.axis_index("dp")
    t = lax.axis_index("tensor")
    core = lax.rem(r, 2)
    chip = r // 2
    x = lax.rem(chip, 4)
    y = chip // 4
    sibling = chip * 2 + (1 - core)

    def act_copy(c):
        rows = pl.ds(pl.multiple_of(c * CH, CH), CH)
        return pltpu.make_async_copy(act_hbm.at[rows], act_v.at[rows], act_sem.at[c])

    def grad_copy(c):
        rows = pl.ds(pl.multiple_of(c * CH, CH), CH)
        return pltpu.make_async_copy(grad_hbm.at[rows], grad_v.at[rows], grad_sem.at[c])

    pin_copy = pltpu.make_async_copy(pin_hbm, pin_v, misc_sem.at[0])
    pout_copy = pltpu.make_async_copy(pout_hbm, pout_v, misc_sem.at[1])
    val_a_copy = pltpu.make_async_copy(
        val_hbm.at[pl.ds(0, 64)], vbuf.at[core, 0, y, x], misc_sem.at[2]
    )
    val_b_copy = pltpu.make_async_copy(
        val_hbm.at[pl.ds(64, 64)], vbuf.at[core, 1, x, y], misc_sem.at[6]
    )
    len_copy = pltpu.make_async_copy(len_hbm, len_v, misc_sem.at[3])
    own_copy = pltpu.make_async_copy(own_hbm, own_v, misc_sem.at[4])

    len_copy.start()
    own_copy.start()
    pin_copy.start()
    act_copy(0).start()
    pout_copy.start()
    grad_copy(0).start()
    val_a_copy.start()
    val_b_copy.start()
    for c in range(1, AHEAD):
        act_copy(c).start()
        grad_copy(c).start()

    barrier = pltpu.get_barrier_semaphore()

    def greet(i, carry):
        other = lax.rem(r + i, ND)
        pl.semaphore_signal(barrier, inc=1, device_id=(other, t), device_id_type=MESH)
        return carry

    lax.fori_loop(1, ND, greet, 0)
    for d in range(1, NT):
        pl.semaphore_signal(
            barrier, inc=1, device_id=(r, lax.rem(t + d, NT)), device_id_type=MESH
        )

    len_copy.wait()
    own_copy.wait()
    lens = len_v[...].astype(F32)
    rows_out = own_v[...]
    owner = rows_out // ND
    slot = (rows_out - owner * ND).astype(F32)
    row_id = lax.broadcasted_iota(jnp.int32, (ND, ND), 0)
    col_id = lax.broadcasted_iota(jnp.int32, (ND, ND), 1)
    chosen = jnp.broadcast_to(owner, (ND, ND)) == row_id
    zero = jnp.zeros((ND, ND), F32)
    doc_at = jnp.sum(jnp.where(chosen, col_id.astype(F32), zero), axis=1, keepdims=True)
    slot_at = jnp.sum(
        jnp.where(chosen, jnp.broadcast_to(slot, (ND, ND)), zero), axis=1, keepdims=True
    )
    lens_all = jnp.broadcast_to(lens, (ND, ND))
    len_at = jnp.sum(jnp.where(chosen, lens_all, zero), axis=1, keepdims=True)
    end_at = jnp.sum(
        jnp.where(col_id.astype(F32) <= doc_at, lens_all, zero), axis=1, keepdims=True
    )
    start_at = end_at - len_at
    params[0] = jnp.broadcast_to(start_at, (ND, 128))
    params[1] = jnp.broadcast_to(end_at, (ND, 128))
    params[2] = jnp.broadcast_to(1.0 / jnp.sqrt(jnp.maximum(len_at, 1.0)), (ND, 128))
    slots_wide = jnp.broadcast_to(slot_at, (ND, 128))
    for i in range(ND):
        lab_out[i] = slots_wide[i : i + 1, :]
    s_ref[...] = jnp.zeros_like(s_ref)

    def multiply(c):
        rows = pl.ds(pl.multiple_of(c * CH, CH), CH)
        act_copy(c).wait()
        grad_copy(c).wait()
        left = lax.dot_general(act_v[rows, :], pin_v[...], NT_DIMS, preferred_element_type=F32)
        right = lax.dot_general(grad_v[rows, :], pout_v[...], NT_DIMS, preferred_element_type=F32)
        part[c] = jnp.concatenate([left, right], axis=1).astype(BF16)

    def scatter_copy(c, d):
        peer = lax.rem(t + d, NT)
        return pltpu.make_async_remote_copy(
            src_ref=part.at[c, pl.ds(pl.multiple_of(peer * SUB, SUB), SUB)],
            dst_ref=rsbuf.at[c, d - 1],
            send_sem=rs_send.at[c],
            recv_sem=rs_recv.at[c],
            device_id=(r, peer),
            device_id_type=MESH,
        )

    def direct_copy(c, d):
        peer = lax.rem(t + d, NT)
        return pltpu.make_async_remote_copy(
            src_ref=part.at[c],
            dst_ref=dbuf.at[c - NRS, d - 1],
            send_sem=rs_send.at[c],
            recv_sem=rs_recv.at[c],
            device_id=(r, peer),
            device_id_type=MESH,
        )

    def gather_copy(c, d):
        peer = lax.rem(t + d, NT)
        mine = full.at[c, pl.ds(pl.multiple_of(t * SUB, SUB), SUB)]
        return pltpu.make_async_remote_copy(
            src_ref=mine,
            dst_ref=mine,
            send_sem=ag_send.at[c],
            recv_sem=ag_recv.at[c],
            device_id=(r, peer),
            device_id_type=MESH,
        )

    def reduce(c):
        bytes_wait(rsbuf.at[c], rs_recv.at[c])
        mine = pl.ds(pl.multiple_of(t * SUB, SUB), SUB)
        total = part[c, mine, :].astype(F32)
        for d in range(NT - 1):
            total = total + rsbuf[c, d].astype(F32)
        full[c, mine, :] = total.astype(BF16)
        for d in (2, 1, 3):
            gather_copy(c, d).start()

    def ahead(c):
        @pl.when(c + (AHEAD - 1) < NCH)
        def _():
            act_copy(c + (AHEAD - 1)).start()
            grad_copy(c + (AHEAD - 1)).start()

    def early(c, carry):
        @pl.when(c > 0)
        def _():
            ahead(c)

        multiply(c)
        return carry

    pin_copy.wait()
    pout_copy.wait()
    lax.fori_loop(0, EARLY, early, 0)
    val_a_copy.wait()
    val_b_copy.wait()
    pl.semaphore_wait(barrier, ND - 1 + NT - 1)
    for d in (2, 1, 3):
        for c in range(EARLY):
            scatter_copy(c, d).start()

    def val_to(peer, send, recv, ref):
        return pltpu.make_async_remote_copy(
            src_ref=ref,
            dst_ref=ref,
            send_sem=send,
            recv_sem=recv,
            device_id=(peer, t),
            device_id_type=MESH,
        )

    def along_x(d):
        return (y * 4 + lax.rem(x + d, 4)) * 2 + core

    def along_y(d):
        return (lax.rem(y + d, 4) * 4 + x) * 2 + core

    for d in (2, 1, 3):
        val_to(along_x(d), v_send.at[0], v_recv.at[0], vbuf.at[core, 0, y, x]).start()
        val_to(along_y(d), v_send.at[1], v_recv.at[1], vbuf.at[core, 1, x, y]).start()

    def lab_copy(i):
        peer = lax.rem(r + i, ND)
        return pltpu.make_async_remote_copy(
            src_ref=lab_out.at[peer],
            dst_ref=lab_in.at[r],
            send_sem=lab_send,
            recv_sem=lab_recv,
            device_id=(peer, t),
            device_id_type=MESH,
        )

    def lab_go(i, carry):
        lab_copy(i).start()
        return carry

    lax.fori_loop(1, ND, lab_go, 0)
    lab_in[r] = lab_out[r]

    def val_second():
        bytes_wait(vbuf.at[0, 0, 0, pl.ds(0, 3)], v_recv.at[0])
        bytes_wait(vbuf.at[0, 0, 0, pl.ds(0, 3)], v_recv.at[1])
        for d in (2, 1, 3):
            val_to(along_y(d), v_send.at[2], v_recv.at[2], vbuf.at[core, 0, y]).start()
            val_to(along_x(d), v_send.at[3], v_recv.at[3], vbuf.at[core, 1, x]).start()

    def step(c, carry):
        ahead(c)
        multiply(c)

        @pl.when(c < NRS)
        def _():
            for d in (2, 1, 3):
                scatter_copy(c, d).start()

        @pl.when(c >= NRS)
        def _():
            for d in (2, 1, 3):
                direct_copy(c, d).start()

        @pl.when(c >= LAG)
        def _():
            reduce(c - LAG)

        @pl.when(c == SECOND)
        def _():
            val_second()

        return carry

    lax.fori_loop(EARLY, NCH, step, 0)
    for c in range(NCH - LAG, NRS):
        reduce(c)

    bytes_wait(lab_in.at[pl.ds(0, ND - 1)], lab_recv)
    slots_in = jnp.concatenate([lab_in[i] for i in range(ND)], axis=0)
    lane = lax.broadcasted_iota(jnp.int32, (ND, 128), 1).astype(F32)
    place = (slots_in == lane).astype(BF16)
    eye = (row_id == col_id).astype(BF16)
    place = lax.dot_general(
        place, eye, (((0,), (0,)), ((), ())), preferred_element_type=F32
    )[0:ND].astype(BF16)
    place_v[...] = place

    lane_a = lax.broadcasted_iota(jnp.int32, (64, 128), 1)
    row_a = lax.broadcasted_iota(jnp.int32, (64, 128), 0)
    pick = jnp.where(row_a < 32, 2 * row_a, 2 * (row_a - 32) + 1)
    spread = (lane_a == pick).astype(BF16)
    low = lax.broadcasted_iota(jnp.int32, (PAIR, 128), 1) < 64

    def sketch(p, total):
        turned = lax.dot_general(
            spread, total.astype(BF16), NT_DIMS, preferred_element_type=F32
        )
        at_ref[:, 0:PAIR] = turned[0:32]
        at_ref[:, PAIR : 2 * PAIR] = turned[32:64]
        rolled = pltpu.roll(total, 64, 1)
        upper = jnp.where(low, rolled, 0.0).astype(BF16)
        lower = jnp.where(low, 0.0, total).astype(BF16)
        rhs = jnp.concatenate([upper, lower], axis=0)
        pos = lax.broadcasted_iota(jnp.int32, (ND, 128), 1).astype(F32)
        pieces = []
        for i in range(PAIR // 128):
            at = pos + jnp.asarray(p * PAIR + i * 128, F32)
            pieces.append(((at >= params[0]) & (at < params[1])).astype(F32))
        member = jnp.concatenate(pieces + pieces, axis=1)
        for k in range(32):
            lhs_ref[k * ND : (k + 1) * ND, :] = (at_ref[k : k + 1, :] * member).astype(BF16)
        s_ref[...] += jnp.dot(lhs_ref[...], rhs, preferred_element_type=F32)

    def summed(c):
        if c < NRS:
            bytes_wait(rsbuf.at[c], ag_recv.at[c])
            return full[c].astype(F32)
        bytes_wait(dbuf.at[c - NRS], rs_recv.at[c])
        total = part[c].astype(F32)
        for d in range(NT - 1):
            total = total + dbuf[c - NRS, d].astype(F32)
        return total

    for p in range(TOKENS_ROW // PAIR):
        if p == MIDDLE:
            bytes_wait(vbuf.at[0, 0, pl.ds(0, 3)], v_recv.at[2])
            bytes_wait(vbuf.at[0, 0, pl.ds(0, 3)], v_recv.at[3])
            val_to(sibling, v_send.at[4], v_recv.at[4], vbuf.at[core]).start()
        each = PAIR // CH
        sketch(p, jnp.concatenate([summed(p * each + i) for i in range(each)], axis=0))

    bytes_wait(vbuf.at[0], v_recv.at[4])
    place_copy = pltpu.make_async_copy(place_v, place_hbm, misc_sem.at[7])
    place_copy.start()
    local = jnp.zeros((ND, 128), F32)
    for k in range(0, 32, 2):
        left = jnp.concatenate(
            [s_ref[k * ND : (k + 1) * ND, :], s_ref[(k + 1) * ND : (k + 2) * ND, :]], axis=1
        ).astype(BF16)
        ky, kx = k // 8, (k // 2) % 4
        right = jnp.concatenate(
            [
                jnp.concatenate([vbuf[j, 0, ky, kx], vbuf[j, 1, kx, ky]], axis=0)
                for j in range(2)
            ],
            axis=1,
        )
        local = local + lax.dot_general(
            left, right, (((1,), (1,)), ((), ())), preferred_element_type=F32
        )
    local = (local * params[2]).astype(BF16)
    for i in range(ND):
        sc_out[i] = local[i : i + 1, :]

    def score_copy(i):
        peer = lax.rem(r + i, ND)
        return pltpu.make_async_remote_copy(
            src_ref=sc_out.at[peer],
            dst_ref=got_hbm.at[r],
            send_sem=sc_send,
            recv_sem=sc_recv,
            device_id=(peer, t),
            device_id_type=MESH,
        )

    def score_go(i, carry):
        score_copy(i).start()
        return carry

    lax.fori_loop(1, ND, score_go, 0)
    own_score = pltpu.make_async_copy(sc_out.at[r], got_hbm.at[r], misc_sem.at[5])
    own_score.start()

    for c in range(NRS):
        bytes_wait(rsbuf.at[c], rs_send.at[c])
        bytes_wait(rsbuf.at[c], ag_send.at[c])
    for c in range(NRS, NCH):
        bytes_wait(dbuf.at[c - NRS], rs_send.at[c])
    for i in range(2):
        bytes_wait(vbuf.at[0, 0, 0, pl.ds(0, 3)], v_send.at[i])
        bytes_wait(vbuf.at[0, 0, pl.ds(0, 3)], v_send.at[2 + i])
    bytes_wait(vbuf.at[0], v_send.at[4])
    bytes_wait(lab_out.at[pl.ds(0, ND - 1)], lab_send)

    bytes_wait(sc_out.at[pl.ds(0, ND - 1)], sc_send)
    own_score.wait()
    place_copy.wait()
    bytes_wait(got_hbm.at[pl.ds(0, ND - 1)], sc_recv)


def shards(activations, out_grads, proj_in, proj_out, validation, doc_lengths, owner_rows):
    tokens, width_in = activations.shape
    width_out = out_grads.shape[1]
    dma = pltpu.SemaphoreType.DMA
    any_spec = pl.BlockSpec(memory_space=pl.ANY)
    got, place = pl.pallas_call(
        kernel,
        out_shape=(
            jax.ShapeDtypeStruct((ND, 1, 128), BF16),
            jax.ShapeDtypeStruct((ND, ND), BF16),
        ),
        in_specs=[any_spec] * 7,
        out_specs=(any_spec, any_spec),
        scratch_shapes=[
            pltpu.VMEM((tokens, width_in), BF16),
            pltpu.VMEM((tokens, width_out), BF16),
            pltpu.VMEM((64, width_in), BF16),
            pltpu.VMEM((64, width_out), BF16),
            pltpu.VMEM((1, ND), jnp.int32),
            pltpu.VMEM((1, ND), jnp.int32),
            pltpu.VMEM((NCH, CH, 128), BF16),
            pltpu.VMEM((NRS, NT - 1, SUB, 128), BF16),
            pltpu.VMEM((NCH - NRS, NT - 1, CH, 128), BF16),
            pltpu.VMEM((NRS, CH, 128), BF16),
            pltpu.VMEM((2, 2, 4, 4, 64, 128), BF16),
            pltpu.VMEM((3, ND, 128), F32),
            pltpu.VMEM((ND, 1, 128), F32),
            pltpu.VMEM((ND, 1, 128), F32),
            pltpu.VMEM((ND, 1, 128), BF16),
            pltpu.VMEM((32, 2 * PAIR), F32),
            pltpu.VMEM((32 * ND, 2 * PAIR), BF16),
            pltpu.VMEM((32 * ND, 128), F32),
            pltpu.VMEM((ND, ND), BF16),
            dma((NCH,)),
            dma((NCH,)),
            dma((8,)),
            dma((5,)),
            dma((5,)),
            dma((NCH,)),
            dma((NCH,)),
            dma((NRS,)),
            dma((NRS,)),
            dma,
            dma,
            dma,
            dma,
        ],
        compiler_params=pltpu.CompilerParams(collective_id=0, has_side_effects=True),
        name="sketch_scores",
    )(activations, out_grads, proj_in.T, proj_out.T, validation, doc_lengths, owner_rows)
    placed = jnp.dot(place, got.reshape(ND, 128), preferred_element_type=F32)
    return placed.astype(BF16)


def solution(mesh):
    placed = (
        P("dp", "tensor"),
        P("dp", "tensor"),
        P("tensor", None),
        P("tensor", None),
        P("tensor", "dp"),
        P("dp", None),
        P("dp", None),
    )
    return jax.shard_map(
        shards, mesh=mesh, in_specs=placed, out_specs=P("dp", "tensor"), check_vma=False
    )
```

```python
import jax
import jax.numpy as jnp
from jax import lax
from jax.experimental import pallas as pl
from jax.experimental.pallas import tpu as pltpu
from jax.sharding import PartitionSpec as P

MESH = pl.DeviceIdType.MESH
F32 = jnp.float32
BF16 = jnp.bfloat16

NT_DIMS = (((1,), (1,)), ((), ()))
CH = 128
NCH = 1024 // CH
NRS = 7
LAG = 4
SECOND = 4
EARLY = 2
MIDDLE = 2
TOKENS_ROW = 1024
PAIR = 256
NT = 4
ND = 32
SUB = CH // NT
HALF = CH // 2
AHEAD = 3


def bytes_wait(ref, sem):
    pltpu.make_async_copy(ref, ref, sem).wait()


def kernel(
    act_hbm, grad_hbm, pin_hbm, pout_hbm, val_hbm, len_hbm, own_hbm, got_hbm, place_hbm,
    act_v, grad_v, pin_v, pout_v, len_v, own_v,
    part, rsbuf, dbuf, full, vbuf, params, lab_out, lab_in, sc_out,
    at_ref, lhs_ref, s_ref, place_v,
    act_sem, grad_sem, misc_sem,
    v_send, v_recv, rs_send, rs_recv, ag_send, ag_recv,
    lab_send, lab_recv, sc_send, sc_recv,
):
    r = lax.axis_index("dp")
    t = lax.axis_index("tensor")
    core = lax.rem(r, 2)
    chip = r // 2
    x = lax.rem(chip, 4)
    y = chip // 4
    sibling = chip * 2 + (1 - core)

    def act_copy(c):
        rows = pl.ds(pl.multiple_of(c * CH, CH), CH)
        return pltpu.make_async_copy(act_hbm.at[rows], act_v.at[rows], act_sem.at[c])

    def grad_copy(c):
        rows = pl.ds(pl.multiple_of(c * CH, CH), CH)
        return pltpu.make_async_copy(grad_hbm.at[rows], grad_v.at[rows], grad_sem.at[c])

    pin_copy = pltpu.make_async_copy(pin_hbm, pin_v, misc_sem.at[0])
    pout_copy = pltpu.make_async_copy(pout_hbm, pout_v, misc_sem.at[1])
    val_a_copy = pltpu.make_async_copy(
        val_hbm.at[pl.ds(0, 64)], vbuf.at[core, 0, y, x], misc_sem.at[2]
    )
    val_b_copy = pltpu.make_async_copy(
        val_hbm.at[pl.ds(64, 64)], vbuf.at[core, 1, x, y], misc_sem.at[6]
    )
    len_copy = pltpu.make_async_copy(len_hbm, len_v, misc_sem.at[3])
    own_copy = pltpu.make_async_copy(own_hbm, own_v, misc_sem.at[4])

    len_copy.start()
    own_copy.start()
    pin_copy.start()
    act_copy(0).start()
    pout_copy.start()
    grad_copy(0).start()
    val_a_copy.start()
    val_b_copy.start()
    for c in range(1, AHEAD):
        act_copy(c).start()
        grad_copy(c).start()

    barrier = pltpu.get_barrier_semaphore()

    def greet(i, carry):
        other = lax.rem(r + i, ND)
        pl.semaphore_signal(barrier, inc=1, device_id=(other, t), device_id_type=MESH)
        return carry

    lax.fori_loop(1, ND, greet, 0)
    for d in range(1, NT):
        pl.semaphore_signal(
            barrier, inc=1, device_id=(r, lax.rem(t + d, NT)), device_id_type=MESH
        )

    len_copy.wait()
    own_copy.wait()
    lens = len_v[...].astype(F32)
    rows_out = own_v[...]
    owner = rows_out // ND
    slot = (rows_out - owner * ND).astype(F32)
    row_id = lax.broadcasted_iota(jnp.int32, (ND, ND), 0)
    col_id = lax.broadcasted_iota(jnp.int32, (ND, ND), 1)
    chosen = jnp.broadcast_to(owner, (ND, ND)) == row_id
    zero = jnp.zeros((ND, ND), F32)
    doc_at = jnp.sum(jnp.where(chosen, col_id.astype(F32), zero), axis=1, keepdims=True)
    slot_at = jnp.sum(
        jnp.where(chosen, jnp.broadcast_to(slot, (ND, ND)), zero), axis=1, keepdims=True
    )
    lens_all = jnp.broadcast_to(lens, (ND, ND))
    len_at = jnp.sum(jnp.where(chosen, lens_all, zero), axis=1, keepdims=True)
    end_at = jnp.sum(
        jnp.where(col_id.astype(F32) <= doc_at, lens_all, zero), axis=1, keepdims=True
    )
    start_at = end_at - len_at
    params[0] = jnp.broadcast_to(start_at, (ND, 128))
    params[1] = jnp.broadcast_to(end_at, (ND, 128))
    params[2] = jnp.broadcast_to(1.0 / jnp.sqrt(jnp.maximum(len_at, 1.0)), (ND, 128))
    slots_wide = jnp.broadcast_to(slot_at, (ND, 128))
    for i in range(ND):
        lab_out[i] = slots_wide[i : i + 1, :]
    s_ref[...] = jnp.zeros_like(s_ref)

    def arrive(c):
        act_copy(c).wait()
        grad_copy(c).wait()

    def multiply(c, first=0, count=CH):
        rows = pl.ds(pl.multiple_of(c * CH + first, count), count)
        left = lax.dot_general(act_v[rows, :], pin_v[...], NT_DIMS, preferred_element_type=F32)
        right = lax.dot_general(grad_v[rows, :], pout_v[...], NT_DIMS, preferred_element_type=F32)
        part[c, first : first + count, :] = jnp.concatenate([left, right], axis=1).astype(BF16)

    def scatter_copy(c, d):
        peer = lax.rem(t + d, NT)
        return pltpu.make_async_remote_copy(
            src_ref=part.at[c, pl.ds(pl.multiple_of(peer * SUB, SUB), SUB)],
            dst_ref=rsbuf.at[c, d - 1],
            send_sem=rs_send.at[c],
            recv_sem=rs_recv.at[c],
            device_id=(r, peer),
            device_id_type=MESH,
        )

    def direct_copy(c, d, half):
        peer = lax.rem(t + d, NT)
        return pltpu.make_async_remote_copy(
            src_ref=part.at[c, pl.ds(half, HALF)],
            dst_ref=dbuf.at[c - NRS, d - 1, pl.ds(half, HALF)],
            send_sem=rs_send.at[c],
            recv_sem=rs_recv.at[c],
            device_id=(r, peer),
            device_id_type=MESH,
        )

    def gather_copy(c, d):
        peer = lax.rem(t + d, NT)
        mine = full.at[c, pl.ds(pl.multiple_of(t * SUB, SUB), SUB)]
        return pltpu.make_async_remote_copy(
            src_ref=mine,
            dst_ref=mine,
            send_sem=ag_send.at[c],
            recv_sem=ag_recv.at[c],
            device_id=(r, peer),
            device_id_type=MESH,
        )

    def reduce(c):
        bytes_wait(rsbuf.at[c], rs_recv.at[c])
        mine = pl.ds(pl.multiple_of(t * SUB, SUB), SUB)
        total = part[c, mine, :].astype(F32)
        for d in range(NT - 1):
            total = total + rsbuf[c, d].astype(F32)
        full[c, mine, :] = total.astype(BF16)
        for d in (2, 1, 3):
            gather_copy(c, d).start()

    def ahead(c):
        @pl.when(c + (AHEAD - 1) < NCH)
        def _():
            act_copy(c + (AHEAD - 1)).start()
            grad_copy(c + (AHEAD - 1)).start()

    def early(c, carry):
        @pl.when(c > 0)
        def _():
            ahead(c)

        arrive(c)
        multiply(c)
        return carry

    pin_copy.wait()
    pout_copy.wait()
    lax.fori_loop(0, EARLY, early, 0)
    val_a_copy.wait()
    val_b_copy.wait()
    pl.semaphore_wait(barrier, ND - 1 + NT - 1)
    for d in (2, 1, 3):
        for c in range(EARLY):
            scatter_copy(c, d).start()

    def val_to(peer, send, recv, ref):
        return pltpu.make_async_remote_copy(
            src_ref=ref,
            dst_ref=ref,
            send_sem=send,
            recv_sem=recv,
            device_id=(peer, t),
            device_id_type=MESH,
        )

    def along_x(d):
        return (y * 4 + lax.rem(x + d, 4)) * 2 + core

    def along_y(d):
        return (lax.rem(y + d, 4) * 4 + x) * 2 + core

    for d in (2, 1, 3):
        val_to(along_x(d), v_send.at[0], v_recv.at[0], vbuf.at[core, 0, y, x]).start()
        val_to(along_y(d), v_send.at[1], v_recv.at[1], vbuf.at[core, 1, x, y]).start()

    def lab_copy(i):
        peer = lax.rem(r + i, ND)
        return pltpu.make_async_remote_copy(
            src_ref=lab_out.at[peer],
            dst_ref=lab_in.at[r],
            send_sem=lab_send,
            recv_sem=lab_recv,
            device_id=(peer, t),
            device_id_type=MESH,
        )

    def lab_go(i, carry):
        lab_copy(i).start()
        return carry

    lax.fori_loop(1, ND, lab_go, 0)
    lab_in[r] = lab_out[r]

    def val_second():
        bytes_wait(vbuf.at[0, 0, 0, pl.ds(0, 3)], v_recv.at[0])
        bytes_wait(vbuf.at[0, 0, 0, pl.ds(0, 3)], v_recv.at[1])
        for d in (2, 1, 3):
            val_to(along_y(d), v_send.at[2], v_recv.at[2], vbuf.at[core, 0, y]).start()
            val_to(along_x(d), v_send.at[3], v_recv.at[3], vbuf.at[core, 1, x]).start()

    def step(c, carry):
        ahead(c)
        arrive(c)
        multiply(c)

        for d in (2, 1, 3):
            scatter_copy(c, d).start()

        @pl.when(c >= LAG)
        def _():
            reduce(c - LAG)

        @pl.when(c == SECOND)
        def _():
            val_second()

        return carry

    lax.fori_loop(EARLY, NRS, step, 0)

    arrive(NRS)
    for half in (0, HALF):
        multiply(NRS, half, HALF)
        for d in (2, 1, 3):
            direct_copy(NRS, d, half).start()
    reduce(NRS - LAG)
    for c in range(NCH - LAG, NRS):
        reduce(c)

    bytes_wait(lab_in.at[pl.ds(0, ND - 1)], lab_recv)
    slots_in = jnp.concatenate([lab_in[i] for i in range(ND)], axis=0)
    lane = lax.broadcasted_iota(jnp.int32, (ND, 128), 1).astype(F32)
    place = (slots_in == lane).astype(BF16)
    eye = (row_id == col_id).astype(BF16)
    place = lax.dot_general(
        place, eye, (((0,), (0,)), ((), ())), preferred_element_type=F32
    )[0:ND].astype(BF16)
    place_v[...] = place

    lane_a = lax.broadcasted_iota(jnp.int32, (64, 128), 1)
    row_a = lax.broadcasted_iota(jnp.int32, (64, 128), 0)
    pick = jnp.where(row_a < 32, 2 * row_a, 2 * (row_a - 32) + 1)
    spread = (lane_a == pick).astype(BF16)
    low = lax.broadcasted_iota(jnp.int32, (PAIR, 128), 1) < 64

    def sketch(p, total):
        turned = lax.dot_general(
            spread, total.astype(BF16), NT_DIMS, preferred_element_type=F32
        )
        at_ref[:, 0:PAIR] = turned[0:32]
        at_ref[:, PAIR : 2 * PAIR] = turned[32:64]
        rolled = pltpu.roll(total, 64, 1)
        upper = jnp.where(low, rolled, 0.0).astype(BF16)
        lower = jnp.where(low, 0.0, total).astype(BF16)
        rhs = jnp.concatenate([upper, lower], axis=0)
        pos = lax.broadcasted_iota(jnp.int32, (ND, 128), 1).astype(F32)
        pieces = []
        for i in range(PAIR // 128):
            at = pos + jnp.asarray(p * PAIR + i * 128, F32)
            pieces.append(((at >= params[0]) & (at < params[1])).astype(F32))
        member = jnp.concatenate(pieces + pieces, axis=1)
        for k in range(32):
            lhs_ref[k * ND : (k + 1) * ND, :] = (at_ref[k : k + 1, :] * member).astype(BF16)
        s_ref[...] += jnp.dot(lhs_ref[...], rhs, preferred_element_type=F32)

    def summed(c):
        if c < NRS:
            bytes_wait(rsbuf.at[c], ag_recv.at[c])
            return full[c].astype(F32)
        bytes_wait(dbuf.at[c - NRS], rs_recv.at[c])
        total = part[c].astype(F32)
        for d in range(NT - 1):
            total = total + dbuf[c - NRS, d].astype(F32)
        return total

    for p in range(TOKENS_ROW // PAIR):
        if p == MIDDLE:
            bytes_wait(vbuf.at[0, 0, pl.ds(0, 3)], v_recv.at[2])
            bytes_wait(vbuf.at[0, 0, pl.ds(0, 3)], v_recv.at[3])
            val_to(sibling, v_send.at[4], v_recv.at[4], vbuf.at[core]).start()
        each = PAIR // CH
        sketch(p, jnp.concatenate([summed(p * each + i) for i in range(each)], axis=0))

    bytes_wait(vbuf.at[0], v_recv.at[4])
    place_copy = pltpu.make_async_copy(place_v, place_hbm, misc_sem.at[7])
    place_copy.start()
    local = jnp.zeros((ND, 128), F32)
    for k in range(0, 32, 2):
        left = jnp.concatenate(
            [s_ref[k * ND : (k + 1) * ND, :], s_ref[(k + 1) * ND : (k + 2) * ND, :]], axis=1
        ).astype(BF16)
        ky, kx = k // 8, (k // 2) % 4
        right = jnp.concatenate(
            [
                jnp.concatenate([vbuf[j, 0, ky, kx], vbuf[j, 1, kx, ky]], axis=0)
                for j in range(2)
            ],
            axis=1,
        )
        local = local + lax.dot_general(
            left, right, (((1,), (1,)), ((), ())), preferred_element_type=F32
        )
    local = (local * params[2]).astype(BF16)
    for i in range(ND):
        sc_out[i] = local[i : i + 1, :]

    def score_copy(i):
        peer = lax.rem(r + i, ND)
        return pltpu.make_async_remote_copy(
            src_ref=sc_out.at[peer],
            dst_ref=got_hbm.at[r],
            send_sem=sc_send,
            recv_sem=sc_recv,
            device_id=(peer, t),
            device_id_type=MESH,
        )

    def score_go(i, carry):
        score_copy(i).start()
        return carry

    lax.fori_loop(1, ND, score_go, 0)
    own_score = pltpu.make_async_copy(sc_out.at[r], got_hbm.at[r], misc_sem.at[5])
    own_score.start()

    for c in range(NRS):
        bytes_wait(rsbuf.at[c], rs_send.at[c])
        bytes_wait(rsbuf.at[c], ag_send.at[c])
    for c in range(NRS, NCH):
        bytes_wait(dbuf.at[c - NRS], rs_send.at[c])
    for i in range(2):
        bytes_wait(vbuf.at[0, 0, 0, pl.ds(0, 3)], v_send.at[i])
        bytes_wait(vbuf.at[0, 0, pl.ds(0, 3)], v_send.at[2 + i])
    bytes_wait(vbuf.at[0], v_send.at[4])
    bytes_wait(lab_out.at[pl.ds(0, ND - 1)], lab_send)

    bytes_wait(sc_out.at[pl.ds(0, ND - 1)], sc_send)
    own_score.wait()
    place_copy.wait()
    bytes_wait(got_hbm.at[pl.ds(0, ND - 1)], sc_recv)


def shards(activations, out_grads, proj_in, proj_out, validation, doc_lengths, owner_rows):
    tokens, width_in = activations.shape
    width_out = out_grads.shape[1]
    dma = pltpu.SemaphoreType.DMA
    any_spec = pl.BlockSpec(memory_space=pl.ANY)
    got, place = pl.pallas_call(
        kernel,
        out_shape=(
            jax.ShapeDtypeStruct((ND, 1, 128), BF16),
            jax.ShapeDtypeStruct((ND, ND), BF16),
        ),
        in_specs=[any_spec] * 7,
        out_specs=(any_spec, any_spec),
        scratch_shapes=[
            pltpu.VMEM((tokens, width_in), BF16),
            pltpu.VMEM((tokens, width_out), BF16),
            pltpu.VMEM((64, width_in), BF16),
            pltpu.VMEM((64, width_out), BF16),
            pltpu.VMEM((1, ND), jnp.int32),
            pltpu.VMEM((1, ND), jnp.int32),
            pltpu.VMEM((NCH, CH, 128), BF16),
            pltpu.VMEM((NRS, NT - 1, SUB, 128), BF16),
            pltpu.VMEM((NCH - NRS, NT - 1, CH, 128), BF16),
            pltpu.VMEM((NRS, CH, 128), BF16),
            pltpu.VMEM((2, 2, 4, 4, 64, 128), BF16),
            pltpu.VMEM((3, ND, 128), F32),
            pltpu.VMEM((ND, 1, 128), F32),
            pltpu.VMEM((ND, 1, 128), F32),
            pltpu.VMEM((ND, 1, 128), BF16),
            pltpu.VMEM((32, 2 * PAIR), F32),
            pltpu.VMEM((32 * ND, 2 * PAIR), BF16),
            pltpu.VMEM((32 * ND, 128), F32),
            pltpu.VMEM((ND, ND), BF16),
            dma((NCH,)),
            dma((NCH,)),
            dma((8,)),
            dma((5,)),
            dma((5,)),
            dma((NCH,)),
            dma((NCH,)),
            dma((NRS,)),
            dma((NRS,)),
            dma,
            dma,
            dma,
            dma,
        ],
        compiler_params=pltpu.CompilerParams(collective_id=0, has_side_effects=True),
        name="sketch_scores",
    )(activations, out_grads, proj_in.T, proj_out.T, validation, doc_lengths, owner_rows)
    placed = jnp.dot(place, got.reshape(ND, 128), preferred_element_type=F32)
    return placed.astype(BF16)


def solution(mesh):
    placed = (
        P("dp", "tensor"),
        P("dp", "tensor"),
        P("tensor", None),
        P("tensor", None),
        P("tensor", "dp"),
        P("dp", None),
        P("dp", None),
    )
    return jax.shard_map(
        shards, mesh=mesh, in_specs=placed, out_specs=P("dp", "tensor"), check_vma=False
    )
```
